32 devices in a mesh: dom: 16 (over z, y, x), tm: 2 (over core).
Axes of the slice: x: 2, y: 2, z: 4, core: 2. Of those that a mesh axis runs over, the one named last changes fastest.
Arguments:
- sources: bfloat16 [256, 3, 16, 256], P('dom', None, 'tm'), may hold values from -6 to 6
- weights: bfloat16 [48, 16, 256, 256], P('dom', None, None, 'tm'), may hold values from -0.09375 to 0.09375
- intersect: int32 [48, 16], replicated, may hold values from 0 to 255, as said below
- block_row: int32 [256], replicated, may hold values from 0 to 255, as said below
- slot_tile: int32 [48], replicated, may hold values from 0 to 47, as said below
Outputs:
- acoustic_source: bfloat16 [48, 3, 16, 256], P('dom', None, 'tm')
- source_rate: bfloat16 [48, 3, 16, 256], P('dom', None, 'tm')
The draws below stay inside these ranges and needn't reach their ends.
Inputs may be any that keep to these rules, and one draw needn't show every extreme that they name: `intersect`: over the 48 links of the slots held by one index of dom, exactly 24 distinct source rows are named, each by exactly two links; no index of dom holds more than 2 of these rows, and some index holds exactly 2. `block_row`: A permutation of the block ids. `slot_tile`: A permutation of the tile ids.
All inputs are finite; a program needn't handle non-finite values.
Results may differ from the reference program's by a relative error of at most 0.007.
Values may be sent and summed in bfloat16 or wider, within the bound.
A program may use at most 64 MiB of HBM per device.

```python
import jax
import jax.numpy as jnp
from jax import lax

CELLS = 256
NODES = 256
COMP = 3
TS = 16
BLK_DEV = 16
TILE_DEV = 3
K = 16
NB = 256
NA = 48
POOL = 24


def link_layout(key):
    domain_count = NB // BLK_DEV
    per_owner = (POOL + domain_count - 1) // domain_count
    slot_count = domain_count * per_owner
    popular = jax.random.randint(jax.random.fold_in(key, 7), (domain_count,), 0, 4).astype(jnp.int32)
    owner_of = jnp.arange(slot_count, dtype=jnp.int32) // per_owner
    within = jnp.arange(slot_count, dtype=jnp.int32) % per_owner

    def device_links(device_key):
        score_key, offset_key, shuffle_key = jax.random.split(device_key, 3)
        jitter = jax.random.randint(score_key, (slot_count,), 0, 4096).astype(jnp.int32)
        scores = (popular[owner_of] * 4096 + jitter) * slot_count + jnp.arange(slot_count, dtype=jnp.int32)
        chosen = jnp.argsort(-scores)[:POOL]
        row_base = jax.random.randint(offset_key, (domain_count,), 0, BLK_DEV).astype(jnp.int32)
        chosen_owner = owner_of[chosen]
        rows_pool = chosen_owner * BLK_DEV + (row_base[chosen_owner] + within[chosen]) % BLK_DEV
        doubled = jnp.concatenate([rows_pool, rows_pool])
        shuffle = jax.random.permutation(shuffle_key, 2 * POOL)
        return doubled[shuffle].reshape(TILE_DEV, K)
    device_keys = jax.random.split(jax.random.fold_in(key, 3), domain_count)
    by_slot = jax.vmap(device_links)(device_keys).reshape(NA, K)
    block_row = jax.random.permutation(jax.random.fold_in(key, 11), NB).astype(jnp.int32)
    row_block = jnp.argsort(block_row).astype(jnp.int32)
    slot_tile = jax.random.permutation(jax.random.fold_in(key, 13), NA).astype(jnp.int32)
    tile_slot = jnp.argsort(slot_tile).astype(jnp.int32)
    intersect = row_block[by_slot][tile_slot]
    return (intersect.astype(jnp.int32), block_row, slot_tile)


def draw_intersect(key, part):
    return link_layout(key)[0]


def draw_block_row(key, part):
    return link_layout(key)[1]


def draw_slot_tile(key, part):
    return link_layout(key)[2]


def block_scale(key, extent, cuts, low, largest):
    gain, own = 1.0, jax.random.fold_in(key, 6)
    for axis_at, blocks in cuts:
        heights = jnp.exp(jax.random.uniform(jax.random.fold_in(own, axis_at), (blocks,), jnp.float32, low / len(cuts), largest / len(cuts)))
        gain = gain * jnp.repeat(heights, extent[axis_at] // blocks).reshape([-1 if axis == axis_at else 1 for axis in range(len(extent))])
    return gain


def noise(key, extent, deviation, limit, cuts=(), kind=jnp.bfloat16):
    values = deviation * jax.random.normal(key, extent, jnp.float32)
    if cuts:
        values = values * block_scale(key, extent, cuts, -0.22, 0.18)
    return jnp.clip(values, -limit, limit).astype(kind)


def setup_inputs(seed: int = 0) -> dict:
    key_list = jax.random.split(jax.random.key(seed), 6)
    return {
        "sources": noise(key_list[0], (NB, COMP, TS, CELLS), 1.0, 6.0, ((0, 16), (2, 2))),
        "weights": noise(key_list[1], (NA, K, CELLS, NODES), (K * CELLS) ** -0.5, 0.09375, ((0, 16), (3, 2))),
        "intersect": draw_intersect(jax.random.fold_in(key_list[5], 71), 0),
        "block_row": draw_block_row(jax.random.fold_in(key_list[5], 71), 0),
        "slot_tile": draw_slot_tile(jax.random.fold_in(key_list[5], 71), 0),
    }


def time_derivative(values):
    central = (values[:, 2:] - values[:, :-2]) * 0.5
    first_edge = values[:, 1:2] - values[:, 0:1]
    last_edge = values[:, -1:] - values[:, -2:-1]
    return jnp.concatenate([first_edge, central, last_edge], axis=1)


def reference(sources, weights, intersect, block_row, slot_tile):
    link_rows = jnp.take(block_row, jnp.take(intersect, slot_tile, axis=0), axis=0).astype(jnp.int32)

    def one_tile(inputs):
        tile_rows, tile_weights = inputs
        picked = jnp.take(sources, tile_rows, axis=0).astype(jnp.float32)
        combined = jnp.einsum("kpsc,kcn->psn", picked, tile_weights.astype(jnp.float32), precision=lax.Precision.HIGHEST)
        return combined.astype(jnp.bfloat16), time_derivative(combined).astype(jnp.bfloat16)

    acoustic_source, source_rate = lax.map(one_tile, (link_rows, weights))
    return acoustic_source, source_rate
```

```python
import functools

import jax
import jax.numpy as jnp
from jax import lax
from jax.experimental import pallas as pl
from jax.experimental.pallas import tpu as pltpu
from jax.sharding import PartitionSpec as P


def tables(sources, weights, intersect, block_row, slot_tile, per_owner, domains):
    me = lax.axis_index("dom")
    blocks = sources.shape[0]
    links = weights.shape[0] * weights.shape[1]
    tile_ids = jnp.arange(intersect.shape[0], dtype=jnp.int32)
    named = jnp.sum(
        jnp.where(slot_tile[:, None, None] == tile_ids[None, :, None], intersect[None], 0), axis=1
    )
    named = named.reshape(domains, links)
    block_ids = jnp.arange(block_row.shape[0], dtype=jnp.int32)
    rows = jnp.sum(jnp.where(named[:, :, None] == block_ids, block_row, 0), axis=2)
    first = me * blocks
    local = rows - first
    mine = (local >= 0) & (local < blocks)
    picks = []
    last = jnp.full((domains, 1), -1, jnp.int32)
    for _ in range(per_owner):
        ahead = jnp.where(mine & (local > last), local, blocks - 1)
        last = jnp.min(ahead, axis=1, keepdims=True)
        picks.append(last)
    send = jnp.concatenate(picks, axis=1).reshape(-1)
    own = lax.dynamic_index_in_dim(rows, me, 0, keepdims=False)
    owner = own // blocks
    below = (owner[:, None] == owner[None, :]) & (own[None, :] < own[:, None])
    rank = jnp.sum(below.astype(jnp.int32), axis=1) // 2
    return send, owner * per_owner + rank


def steps(count, body):
    if count <= 16:
        for i in range(count):
            body(i)
    else:
        def step(i, carry):
            body(i)
            return carry
        lax.fori_loop(0, count, step, 0)


def kernel(
    domains, per_owner,
    send_ref, link_ref, src_ref, w_hbm, out_ref, rate_ref,
    w_ref, pack, buf, stage, land,
    w_sem, send_sem, recv_sem, fsend_sem, frecv_sem, osend_sem, orecv_sem,
):
    me = lax.axis_index("dom")
    core = lax.axis_index("tm")
    other = 1 - core
    tiles, link_count = w_ref.shape[0], w_ref.shape[1]
    mesh_type = pl.DeviceIdType.MESH

    def offset(i):
        return domains // 2 + ((i + 1) // 2) * (1 - 2 * (i % 2))

    barrier = pltpu.get_barrier_semaphore()

    def greet(i):
        to = lax.rem(me + i + 1, domains)
        pl.semaphore_signal(barrier, inc=1, device_id=(to, core), device_id_type=mesh_type)

    steps(domains - 1, greet)
    pl.semaphore_signal(barrier, inc=1, device_id=(me, other), device_id_type=mesh_type)

    loads = [pltpu.make_async_copy(w_hbm.at[t], w_ref.at[t], w_sem.at[t]) for t in range(tiles)]
    for load in loads:
        load.start()

    def fill(d):
        for j in range(per_owner):
            pack[d, j] = src_ref[send_ref[d * per_owner + j]]

    steps(domains, fill)
    for j in range(per_owner):
        buf[core, me * per_owner + j] = src_ref[send_ref[me * per_owner + j]]

    pl.semaphore_wait(barrier, domains)

    def exchange(to, frm):
        return pltpu.make_async_remote_copy(
            src_ref=pack.at[to],
            dst_ref=buf.at[core, pl.ds(frm * per_owner, per_owner)],
            send_sem=send_sem.at[to],
            recv_sem=recv_sem.at[frm],
            device_id=(to, core),
            device_id_type=mesh_type,
        )

    def send(i):
        exchange(lax.rem(me + offset(i), domains), me).start()

    steps(domains - 1, send)

    def forward(source, frm):
        return pltpu.make_async_remote_copy(
            src_ref=source,
            dst_ref=buf.at[core, pl.ds(frm * per_owner, per_owner)],
            send_sem=fsend_sem.at[frm],
            recv_sem=frecv_sem.at[frm],
            device_id=(me, other),
            device_id_type=mesh_type,
        )

    def landed(frm):
        return pltpu.make_async_remote_copy(
            src_ref=pack.at[0],
            dst_ref=buf.at[other, pl.ds(frm * per_owner, per_owner)],
            send_sem=fsend_sem.at[frm],
            recv_sem=frecv_sem.at[frm],
            device_id=(me, other),
            device_id_type=mesh_type,
        )

    forward(pack.at[me], me).start()

    def arrive(i):
        frm = lax.rem(me - offset(i) + domains, domains)
        incoming = pltpu.make_async_remote_copy(
            src_ref=pack.at[0],
            dst_ref=buf.at[core, pl.ds(frm * per_owner, per_owner)],
            send_sem=send_sem.at[frm],
            recv_sem=recv_sem.at[frm],
            device_id=(frm, core),
            device_id_type=mesh_type,
        )
        incoming.wait_recv()
        forward(buf.at[core, pl.ds(frm * per_owner, per_owner)], frm).start()

    steps(domains - 1, arrive)
    steps(domains, lambda d: landed(d).wait_recv())
    for load in loads:
        load.wait()

    swaps = []
    comps, half = src_ref.shape[1], src_ref.shape[2]
    span = 2 * half
    count = comps * span
    width = w_ref.shape[3]
    sample = lax.rem(lax.broadcasted_iota(jnp.int32, (count, width), 0), span)
    mine = pl.ds(pl.multiple_of(core * width, width), width)
    theirs = pl.ds(pl.multiple_of(other * width, width), width)
    for t in range(tiles):
        total = jnp.zeros((count, width), jnp.float32)
        for k in range(link_count):
            slot = link_ref[t * link_count + k]
            early = buf[0, slot].astype(jnp.float32)
            late = buf[1, slot].astype(jnp.float32)
            parts = []
            for p in range(comps):
                parts += [early[p], late[p]]
            lhs = jnp.concatenate(parts, axis=0).astype(jnp.bfloat16)
            total += jnp.dot(lhs, w_ref[t, k], preferred_element_type=jnp.float32)
        later = pltpu.roll(total, count - 1, 0)
        prior = pltpu.roll(total, 1, 0)
        rate = jnp.where(
            sample == 0,
            later - total,
            jnp.where(sample == span - 1, total - prior, (later - prior) * 0.5),
        )
        for which, value, target in ((0, total, out_ref), (1, rate, rate_ref)):
            value = value.reshape(comps, 2, half, width)
            lower, upper = value[:, 0], value[:, 1]
            target[t, :, :, mine] = jnp.where(core == 0, lower, upper).astype(jnp.bfloat16)
            stage[t, which] = jnp.where(core == 0, upper, lower).astype(jnp.bfloat16)
        swap = pltpu.make_async_remote_copy(
            src_ref=stage.at[t],
            dst_ref=land.at[t],
            send_sem=osend_sem.at[t],
            recv_sem=orecv_sem.at[t],
            device_id=(me, other),
            device_id_type=mesh_type,
        )
        swap.start()
        swaps.append(swap)

    def drain(i):
        exchange(lax.rem(me + i + 1, domains), me).wait_send()

    steps(domains - 1, drain)
    steps(domains, lambda d: forward(buf.at[core, pl.ds(0, per_owner)], d).wait_send())
    for t in range(tiles):
        swaps[t].wait()
        out_ref[t, :, :, theirs] = land[t, 0]
        rate_ref[t, :, :, theirs] = land[t, 1]


def shards(sources, weights, intersect, block_row, slot_tile):
    domains = lax.axis_size("dom")
    tiles, link_count, cells, width = weights.shape
    blocks, comps, half, _ = sources.shape
    pool = tiles * link_count // 2
    per_owner = (pool + domains - 1) // domains
    send, link = tables(
        sources, weights, intersect, block_row, slot_tile, per_owner, domains
    )
    vmem, smem = pltpu.VMEM, pltpu.SMEM
    out = jax.ShapeDtypeStruct((tiles, comps, half, 2 * width), jnp.bfloat16)
    block = (comps, half, cells)
    dma = pltpu.SemaphoreType.DMA
    return pl.pallas_call(
        functools.partial(kernel, domains, per_owner),
        out_shape=(out, out),
        in_specs=[
            pl.BlockSpec(memory_space=smem),
            pl.BlockSpec(memory_space=smem),
            pl.BlockSpec(memory_space=vmem),
            pl.BlockSpec(memory_space=pl.ANY),
        ],
        out_specs=(pl.BlockSpec(memory_space=vmem),) * 2,
        scratch_shapes=[
            vmem((tiles, link_count, cells, width), jnp.bfloat16),
            vmem((domains, per_owner) + block, jnp.bfloat16),
            vmem((2, domains * per_owner) + block, jnp.bfloat16),
            vmem((tiles, 2, comps, half, width), jnp.bfloat16),
            vmem((tiles, 2, comps, half, width), jnp.bfloat16),
            dma((tiles,)),
            dma((domains,)),
            dma((domains,)),
            dma((domains,)),
            dma((domains,)),
            dma((tiles,)),
            dma((tiles,)),
        ],
        compiler_params=pltpu.CompilerParams(collective_id=0, has_side_effects=True),
        cost_estimate=pl.CostEstimate(
            flops=4 * comps * half * weights.size, bytes_accessed=2 * weights.size, transcendentals=0
        ),
    )(send, link, sources, weights)


def solution(mesh):
    return jax.shard_map(
        shards,
        mesh=mesh,
        in_specs=(P("dom", None, "tm", None), P("dom", None, None, "tm"), P(), P(), P()),
        out_specs=(P("dom", None, "tm", None), P("dom", None, "tm", None)),
        check_vma=False,
    )
```

```python
import functools

import jax
import jax.numpy as jnp
from jax import lax
from jax.experimental import pallas as pl
from jax.experimental.pallas import tpu as pltpu
from jax.sharding import PartitionSpec as P


BIG = 1 << 30


def lookup(table, index):
    lanes = 128
    within, group = index & (lanes - 1), index >> 7
    outs = []
    for at in range(0, index.shape[1], lanes):
        value = jnp.zeros((index.shape[0], lanes), jnp.int32)
        for g in range(table.shape[1] // lanes):
            got = jnp.take_along_axis(
                table[:, g * lanes : (g + 1) * lanes],
                within[:, at : at + lanes],
                axis=1,
                mode="promise_in_bounds",
            )
            value = jnp.where(group[:, at : at + lanes] == g, got, value)
        outs.append(value)
    return outs[0] if len(outs) == 1 else jnp.concatenate(outs, axis=1)


def steps(count, body):
    if count <= 16:
        for i in range(count):
            body(i)
    else:
        def step(i, carry):
            body(i)
            return carry
        lax.fori_loop(0, count, step, 0)


def kernel(
    domains, per_owner,
    tile_ref, row_ref, cross_ref, src_ref, w_hbm, out_ref,
    wide_tile, wide_row, wide_cross, send_to, link_one, link_two,
    w_ref, pack, buf, acc, stage, land,
    w_sem, send_sem, recv_sem, fsend_sem, frecv_sem, osend_sem, orecv_sem,
):
    me = lax.axis_index("dom")
    core = lax.axis_index("tm")
    other = 1 - core
    links, width = w_ref.shape[0], w_ref.shape[2]
    blocks, comps, half, cells = src_ref.shape
    tiles = acc.shape[0]
    link_count = links // tiles
    span = 2 * half
    count = comps * span
    mesh_type = pl.DeviceIdType.MESH

    def offset(i):
        return domains // 2 + ((i + 1) // 2) * (1 - 2 * (i % 2))

    barrier = pltpu.get_barrier_semaphore()

    def greet(i):
        to = lax.rem(me + i + 1, domains)
        pl.semaphore_signal(barrier, inc=1, device_id=(to, core), device_id_type=mesh_type)

    steps(domains - 1, greet)
    pl.semaphore_signal(barrier, inc=1, device_id=(me, other), device_id_type=mesh_type)

    loads = [
        pltpu.make_async_copy(
            w_hbm.at[pl.ds(t * link_count, link_count)],
            w_ref.at[pl.ds(t * link_count, link_count)],
            w_sem.at[t],
        )
        for t in range(tiles)
    ]
    for load in loads:
        load.start()

    wide_tile[...] = jnp.zeros_like(wide_tile)
    wide_cross[...] = jnp.zeros_like(wide_cross)
    wide_row[...] = jnp.zeros_like(wide_row)
    wide_tile[:, : tile_ref.shape[1]] = jnp.broadcast_to(
        tile_ref[...], (link_count, tile_ref.shape[1])
    )
    wide_cross[:, : cross_ref.shape[1]] = cross_ref[...]
    wide_row[:, : row_ref.shape[1]] = jnp.broadcast_to(
        row_ref[...], (link_count, row_ref.shape[1])
    )
    rows = lookup(wide_row[...], lookup(wide_cross[...], wide_tile[...]))

    slots = rows.shape[1]
    lane = lax.broadcasted_iota(jnp.int32, (1, slots), 1)
    place = lax.rem(lane, tiles)
    local = rows - me * blocks
    mine = (local >= 0) & (local < blocks)
    last = jnp.full((1, slots), -1, jnp.int32)
    for j in range(per_owner):
        least = jnp.min(jnp.where(mine & (local > last), local, BIG), axis=0, keepdims=True)
        joint = least
        for t in range(1, tiles):
            joint = jnp.minimum(joint, pltpu.roll(least, slots - t, 1))
        last = joint
        for t in range(1, tiles):
            last = jnp.where(place == t, pltpu.roll(joint, t, 1), last)
        index = jnp.minimum(last, blocks - 1)
        for d in range(domains):
            send_to[d * per_owner + j] = index[0, d * tiles]

    def fill(d):
        for j in range(per_owner):
            pack[d, j] = src_ref[send_to[d * per_owner + j]]

    steps(domains, fill)
    for j in range(per_owner):
        buf[core, me * per_owner + j] = src_ref[send_to[me * per_owner + j]]

    pl.semaphore_wait(barrier, domains)

    def exchange(to, frm):
        return pltpu.make_async_remote_copy(
            src_ref=pack.at[to],
            dst_ref=buf.at[core, pl.ds(frm * per_owner, per_owner)],
            send_sem=send_sem.at[to],
            recv_sem=recv_sem.at[frm],
            device_id=(to, core),
            device_id_type=mesh_type,
        )

    def send(i):
        exchange(lax.rem(me + offset(i), domains), me).start()

    steps(domains - 1, send)

    def forward(source, frm):
        return pltpu.make_async_remote_copy(
            src_ref=source,
            dst_ref=buf.at[core, pl.ds(frm * per_owner, per_owner)],
            send_sem=fsend_sem.at[frm],
            recv_sem=frecv_sem.at[frm],
            device_id=(me, other),
            device_id_type=mesh_type,
        )

    def landed(frm):
        return pltpu.make_async_remote_copy(
            src_ref=pack.at[0],
            dst_ref=buf.at[other, pl.ds(frm * per_owner, per_owner)],
            send_sem=fsend_sem.at[frm],
            recv_sem=frecv_sem.at[frm],
            device_id=(me, other),
            device_id_type=mesh_type,
        )

    forward(pack.at[me], me).start()

    owners = -(-domains // 128) * 128
    around = lax.broadcasted_iota(jnp.int32, (1, owners), 1)
    owner = around + me
    owner = jnp.where(owner >= domains, owner - domains, owner)
    link = lax.broadcasted_iota(jnp.int32, (link_count, owners), 0)
    locals_ = []
    for t in range(tiles):
        column = jnp.sum(jnp.where(lane == me * tiles + t, rows, 0), axis=1, keepdims=True)
        at = column - owner * blocks
        locals_.append(jnp.where((at >= 0) & (at < blocks), at, BIG))
    last = jnp.full((1, owners), -1, jnp.int32)
    for j in range(per_owner):
        least = [jnp.where(at > last, at, BIG) for at in locals_]
        last = jnp.min(functools.reduce(jnp.minimum, least), axis=0, keepdims=True)
        one = jnp.full((link_count, owners), BIG, jnp.int32)
        two = jnp.full((link_count, owners), -1, jnp.int32)
        for t in range(tiles):
            hit = (locals_[t] == last) & (last < BIG)
            one = jnp.minimum(one, jnp.where(hit, link + t * link_count, BIG))
            two = jnp.maximum(two, jnp.where(hit, link + t * link_count, -1))
        one = jnp.min(one, axis=0, keepdims=True)
        two = jnp.max(two, axis=0, keepdims=True)
        for i in range(domains):
            link_one[i * per_owner + j] = one[0, i]
            link_two[i * per_owner + j] = two[0, i]

    acc[...] = jnp.zeros_like(acc)
    for load in loads:
        load.wait()

    def product(i):
        frm = lax.rem(me + i, domains)
        landed(frm).wait_recv()
        for j in range(per_owner):
            early = buf[0, frm * per_owner + j].astype(jnp.float32)
            late = buf[1, frm * per_owner + j].astype(jnp.float32)
            parts = []
            for p in range(comps):
                parts += [early[p], late[p]]
            lhs = jnp.concatenate(parts, axis=0).astype(jnp.bfloat16)
            one = link_one[i * per_owner + j]
            two = link_two[i * per_owner + j]
            pair = jnp.concatenate(
                [w_ref[jnp.minimum(one, links - 1)], w_ref[jnp.maximum(two, 0)]], axis=1
            )
            both = jnp.dot(lhs, pair, preferred_element_type=jnp.float32)
            for t in range(tiles):
                first, end = t * link_count, (t + 1) * link_count
                acc[t] += jnp.where((one >= first) & (one < end), both[:, :width], 0.0) + jnp.where(
                    (two >= first) & (two < end), both[:, width:], 0.0
                )

    def arrive(i):
        frm = lax.rem(me - offset(i) + domains, domains)
        incoming = pltpu.make_async_remote_copy(
            src_ref=pack.at[0],
            dst_ref=buf.at[core, pl.ds(frm * per_owner, per_owner)],
            send_sem=send_sem.at[frm],
            recv_sem=recv_sem.at[frm],
            device_id=(frm, core),
            device_id_type=mesh_type,
        )
        incoming.wait_recv()
        forward(buf.at[core, pl.ds(frm * per_owner, per_owner)], frm).start()

    lag = 2

    def both_steps(i):
        if isinstance(i, int):
            if i < domains - 1:
                arrive(i)
            if i == 0:
                product(0)
            if i >= lag:
                product(domains - offset(i - lag))

    if domains <= 16:
        for i in range(domains - 1 + lag):
            both_steps(i)
    else:
        steps(domains - 1, arrive)
        steps(domains, product)

    sample = lax.rem(lax.broadcasted_iota(jnp.int32, (count, width), 0), span)
    mine = pl.ds(pl.multiple_of(core * width, width), width)
    theirs = pl.ds(pl.multiple_of(other * width, width), width)
    swaps = []
    for t in range(tiles):
        total = acc[t]
        later = pltpu.roll(total, count - 1, 0)
        prior = pltpu.roll(total, 1, 0)
        rate = jnp.where(
            sample == 0,
            later - total,
            jnp.where(sample == span - 1, total - prior, (later - prior) * 0.5),
        )
        for which, value in ((0, total), (1, rate)):
            value = value.reshape(comps, 2, half, width)
            lower, upper = value[:, 0], value[:, 1]
            out_ref[which, t, :, :, mine] = jnp.where(core == 0, lower, upper).astype(jnp.bfloat16)
            stage[t, which] = jnp.where(core == 0, upper, lower).astype(jnp.bfloat16)
    for t in range(tiles):
        swap = pltpu.make_async_remote_copy(
            src_ref=stage.at[t],
            dst_ref=land.at[t],
            send_sem=osend_sem.at[t],
            recv_sem=orecv_sem.at[t],
            device_id=(me, other),
            device_id_type=mesh_type,
        )
        swap.start()
        swaps.append(swap)

    def drain(i):
        exchange(lax.rem(me + i + 1, domains), me).wait_send()

    steps(domains - 1, drain)
    steps(domains, lambda d: forward(buf.at[core, pl.ds(0, per_owner)], d).wait_send())
    for t in range(tiles):
        swaps[t].wait()
        for which in range(2):
            out_ref[which, t, :, :, theirs] = land[t, which]


def deliver(both_ref, source_ref, rate_ref):
    source_ref[...] = both_ref[0]
    rate_ref[...] = both_ref[1]


def shards(sources, weights, intersect, block_row, slot_tile):
    domains = lax.axis_size("dom")
    tiles, link_count, cells, width = weights.shape
    blocks, comps, half, _ = sources.shape
    links = tiles * link_count
    pool = links // 2
    per_owner = (pool + domains - 1) // domains
    vmem, smem = pltpu.VMEM, pltpu.SMEM
    shape = (tiles, comps, half, 2 * width)
    out = jax.ShapeDtypeStruct(shape, jnp.bfloat16)
    block = (comps, half, cells)
    dma = pltpu.SemaphoreType.DMA
    in_vmem = pl.BlockSpec(memory_space=vmem)

    def wide(n):
        return vmem((link_count, -(-n // 128) * 128), jnp.int32)

    both = pl.pallas_call(
        functools.partial(kernel, domains, per_owner),
        out_shape=jax.ShapeDtypeStruct((2,) + shape, jnp.bfloat16),
        in_specs=[in_vmem, in_vmem, in_vmem, in_vmem, pl.BlockSpec(memory_space=pl.ANY)],
        out_specs=in_vmem,
        scratch_shapes=[
            wide(slot_tile.shape[0]),
            wide(block_row.shape[0]),
            wide(intersect.shape[0]),
            smem((domains * per_owner,), jnp.int32),
            smem((domains * per_owner,), jnp.int32),
            smem((domains * per_owner,), jnp.int32),
            vmem((links, cells, width), jnp.bfloat16),
            vmem((domains, per_owner) + block, jnp.bfloat16),
            vmem((2, domains * per_owner) + block, jnp.bfloat16),
            vmem((tiles, 2 * comps * half, width), jnp.float32),
            vmem((tiles, 2, comps, half, width), jnp.bfloat16),
            vmem((tiles, 2, comps, half, width), jnp.bfloat16),
            dma((tiles,)),
            dma((domains,)),
            dma((domains,)),
            dma((domains,)),
            dma((domains,)),
            dma((tiles,)),
            dma((tiles,)),
        ],
        compiler_params=pltpu.CompilerParams(collective_id=0, has_side_effects=True),
        cost_estimate=pl.CostEstimate(
            flops=4 * comps * half * weights.size,
            bytes_accessed=2 * weights.size,
            transcendentals=0,
        ),
    )(
        slot_tile.reshape(1, -1),
        block_row.reshape(1, -1),
        intersect.T,
        sources,
        weights.reshape(links, cells, width),
    )
    return pl.pallas_call(
        deliver,
        out_shape=(out, out),
        in_specs=[in_vmem],
        out_specs=(in_vmem, in_vmem),
    )(both)


def solution(mesh):
    return jax.shard_map(
        shards,
        mesh=mesh,
        in_specs=(P("dom", None, "tm", None), P("dom", None, None, "tm"), P(), P(), P()),
        out_specs=(P("dom", None, "tm", None), P("dom", None, "tm", None)),
        check_vma=False,
    )
```

```python
import functools

import jax
import jax.numpy as jnp
from jax import lax
from jax.experimental import pallas as pl
from jax.experimental.pallas import tpu as pltpu
from jax.sharding import PartitionSpec as P


BIG = 1 << 30


def lookup(table, index):
    lanes = 128
    within, group = index & (lanes - 1), index >> 7
    outs = []
    for at in range(0, index.shape[1], lanes):
        value = jnp.zeros((index.shape[0], lanes), jnp.int32)
        for g in range(table.shape[1] // lanes):
            got = jnp.take_along_axis(
                table[:, g * lanes : (g + 1) * lanes],
                within[:, at : at + lanes],
                axis=1,
                mode="promise_in_bounds",
            )
            value = jnp.where(group[:, at : at + lanes] == g, got, value)
        outs.append(value)
    return outs[0] if len(outs) == 1 else jnp.concatenate(outs, axis=1)


def steps(count, body):
    if count <= 16:
        for i in range(count):
            body(i)
    else:
        def step(i, carry):
            body(i)
            return carry
        lax.fori_loop(0, count, step, 0)


def kernel(
    domains, per_owner,
    tile_hbm, row_hbm, cross_hbm, src_hbm, w_hbm, out_ref,
    tile_ref, row_ref, cross_ref, src_ref,
    wide_tile, wide_row, wide_cross, send_to, link_one, link_two,
    w_ref, pack, buf, acc, edge, beyond,
    in_sem, w_sem, send_sem, recv_sem, wsend_sem, wrecv_sem, edge_sem,
):
    me = lax.axis_index("dom")
    core = lax.axis_index("tm")
    other = 1 - core
    links, width = w_ref.shape[1], w_ref.shape[3]
    blocks, comps, half, cells = src_ref.shape
    tiles = acc.shape[0]
    link_count = links // tiles
    count = comps * half
    mesh_type = pl.DeviceIdType.MESH

    def offset(i):
        return domains // 2 + ((i + 1) // 2) * (1 - 2 * (i % 2))

    barrier = pltpu.get_barrier_semaphore()

    def greet(i):
        to = lax.rem(me + i + 1, domains)
        pl.semaphore_signal(barrier, inc=1, device_id=(to, core), device_id_type=mesh_type)

    steps(domains - 1, greet)
    pl.semaphore_signal(barrier, inc=1, device_id=(me, other), device_id_type=mesh_type)

    inputs = [
        pltpu.make_async_copy(source, target, in_sem.at[i])
        for i, (source, target) in enumerate(
            (
                (cross_hbm, cross_ref),
                (tile_hbm, tile_ref),
                (row_hbm, row_ref),
                (src_hbm, src_ref),
            )
        )
    ]
    for load in inputs:
        load.start()
    parts = [pl.ds(t * link_count, link_count) for t in range(tiles)]
    loads = [
        pltpu.make_async_copy(w_hbm.at[part], w_ref.at[core, part], w_sem.at[t])
        for t, part in enumerate(parts)
    ]
    for load in loads:
        load.start()

    wide_tile[...] = jnp.zeros_like(wide_tile)
    wide_cross[...] = jnp.zeros_like(wide_cross)
    wide_row[...] = jnp.zeros_like(wide_row)
    for load in inputs[:3]:
        load.wait()
    wide_tile[:, : tile_ref.shape[1]] = jnp.broadcast_to(
        tile_ref[...], (link_count, tile_ref.shape[1])
    )
    wide_cross[:, : cross_ref.shape[1]] = cross_ref[...]
    wide_row[:, : row_ref.shape[1]] = jnp.broadcast_to(
        row_ref[...], (link_count, row_ref.shape[1])
    )
    rows = lookup(wide_row[...], lookup(wide_cross[...], wide_tile[...]))

    slots = rows.shape[1]
    lane = lax.broadcasted_iota(jnp.int32, (1, slots), 1)
    place = lax.rem(lane, tiles)
    local = rows - me * blocks
    mine = (local >= 0) & (local < blocks)
    last = jnp.full((1, slots), -1, jnp.int32)
    for j in range(per_owner):
        least = jnp.min(jnp.where(mine & (local > last), local, BIG), axis=0, keepdims=True)
        joint = least
        for t in range(1, tiles):
            joint = jnp.minimum(joint, pltpu.roll(least, slots - t, 1))
        last = joint
        for t in range(1, tiles):
            last = jnp.where(place == t, pltpu.roll(joint, t, 1), last)
        index = jnp.minimum(last, blocks - 1)
        for d in range(domains):
            send_to[d * per_owner + j] = index[0, d * tiles]

    def fill(d):
        for j in range(per_owner):
            pack[d, j] = src_ref[send_to[d * per_owner + j]]

    inputs[3].wait()
    steps(domains, fill)
    for j in range(per_owner):
        buf[me * per_owner + j] = src_ref[send_to[me * per_owner + j]]

    pl.semaphore_wait(barrier, domains)

    def exchange(to, frm):
        return pltpu.make_async_remote_copy(
            src_ref=pack.at[to],
            dst_ref=buf.at[pl.ds(frm * per_owner, per_owner)],
            send_sem=send_sem.at[to],
            recv_sem=recv_sem.at[frm],
            device_id=(to, core),
            device_id_type=mesh_type,
        )

    def send(i):
        exchange(lax.rem(me + offset(i), domains), me).start()

    steps(domains - 1, send)

    swaps = [
        pltpu.make_async_remote_copy(
            src_ref=w_hbm.at[part],
            dst_ref=w_ref.at[core, part],
            send_sem=wsend_sem.at[t],
            recv_sem=wrecv_sem.at[t],
            device_id=(me, other),
            device_id_type=mesh_type,
        )
        for t, part in enumerate(parts)
    ]
    for swap in swaps:
        swap.start()

    owners = -(-domains // 128) * 128
    around = lax.broadcasted_iota(jnp.int32, (1, owners), 1)
    owner = around + me
    owner = jnp.where(owner >= domains, owner - domains, owner)
    link = lax.broadcasted_iota(jnp.int32, (link_count, owners), 0)
    locals_ = []
    for t in range(tiles):
        column = jnp.sum(jnp.where(lane == me * tiles + t, rows, 0), axis=1, keepdims=True)
        at = column - owner * blocks
        locals_.append(jnp.where((at >= 0) & (at < blocks), at, BIG))
    last = jnp.full((1, owners), -1, jnp.int32)
    for j in range(per_owner):
        least = [jnp.where(at > last, at, BIG) for at in locals_]
        last = jnp.min(functools.reduce(jnp.minimum, least), axis=0, keepdims=True)
        one = jnp.full((link_count, owners), BIG, jnp.int32)
        two = jnp.full((link_count, owners), -1, jnp.int32)
        for t in range(tiles):
            hit = (locals_[t] == last) & (last < BIG)
            one = jnp.minimum(one, jnp.where(hit, link + t * link_count, BIG))
            two = jnp.maximum(two, jnp.where(hit, link + t * link_count, -1))
        one = jnp.min(one, axis=0, keepdims=True)
        two = jnp.max(two, axis=0, keepdims=True)
        for i in range(domains):
            link_one[i * per_owner + j] = one[0, i]
            link_two[i * per_owner + j] = two[0, i]

    acc[...] = jnp.zeros_like(acc)
    def product(i):
        frm = lax.rem(me + i, domains)
        for j in range(per_owner):
            rows_here = buf[frm * per_owner + j].astype(jnp.float32)
            lhs = rows_here.reshape(count, cells).astype(jnp.bfloat16)
            one = link_one[i * per_owner + j]
            two = link_two[i * per_owner + j]
            at_one, at_two = jnp.minimum(one, links - 1), jnp.maximum(two, 0)
            quad = jnp.concatenate(
                [w_ref[0, at_one], w_ref[1, at_one], w_ref[0, at_two], w_ref[1, at_two]], axis=1
            )
            both = jnp.dot(lhs, quad, preferred_element_type=jnp.float32)
            for t in range(tiles):
                first, end = t * link_count, (t + 1) * link_count
                acc[t] += jnp.where(
                    (one >= first) & (one < end), both[:, : 2 * width], 0.0
                ) + jnp.where((two >= first) & (two < end), both[:, 2 * width :], 0.0)

    def arrive(i):
        frm = lax.rem(me - offset(i) + domains, domains)
        incoming = pltpu.make_async_remote_copy(
            src_ref=pack.at[0],
            dst_ref=buf.at[pl.ds(frm * per_owner, per_owner)],
            send_sem=send_sem.at[frm],
            recv_sem=recv_sem.at[frm],
            device_id=(frm, core),
            device_id_type=mesh_type,
        )
        incoming.wait_recv()

    def weights_in():
        for load in loads:
            load.wait()
        for t, part in enumerate(parts):
            pltpu.make_async_remote_copy(
                src_ref=w_hbm.at[part],
                dst_ref=w_ref.at[other, part],
                send_sem=wsend_sem.at[t],
                recv_sem=wrecv_sem.at[t],
                device_id=(me, other),
                device_id_type=mesh_type,
            ).wait_recv()

    weights_in()
    product(0)
    if domains <= 16:
        for i in range(domains - 1):
            arrive(i)
            product(domains - offset(i))
    else:
        steps(domains - 1, arrive)
        steps(domains - 1, lambda i: product(i + 1))

    total = acc[...].reshape(tiles, comps, half, 2 * width)
    edge[...] = jnp.where(core == 0, total[:, :, half - 1], total[:, :, 0])
    halo = pltpu.make_async_remote_copy(
        src_ref=edge,
        dst_ref=beyond,
        send_sem=edge_sem.at[0],
        recv_sem=edge_sem.at[1],
        device_id=(me, other),
        device_id_type=mesh_type,
    )
    out_ref[0] = total.astype(jnp.bfloat16)

    def drain(i):
        exchange(lax.rem(me + i + 1, domains), me).wait_send()

    steps(domains - 1, drain)
    for swap in swaps:
        swap.wait_send()
    halo.start()
    halo.wait()
    sample = lax.broadcasted_iota(jnp.int32, (half, 2 * width), 0)
    for t in range(tiles):
        for p in range(comps):
            here = total[t, p]
            outer = jnp.broadcast_to(beyond[t, pl.ds(p, 1)], here.shape)
            later = pltpu.roll(here, half - 1, 0)
            prior = pltpu.roll(here, 1, 0)
            later = jnp.where((sample == half - 1) & (core == 0), outer, later)
            prior = jnp.where((sample == 0) & (core == 1), outer, prior)
            rate = jnp.where(
                (sample == 0) & (core == 0),
                later - here,
                jnp.where(
                    (sample == half - 1) & (core == 1), here - prior, (later - prior) * 0.5
                ),
            )
            out_ref[1, t, p] = rate.astype(jnp.bfloat16)


def deliver(both_ref, source_ref, rate_ref):
    source_ref[...] = both_ref[0]
    rate_ref[...] = both_ref[1]


def shards(sources, weights, intersect, block_row, slot_tile):
    domains = lax.axis_size("dom")
    tiles, link_count, cells, width = weights.shape
    blocks, comps, half, _ = sources.shape
    links = tiles * link_count
    pool = links // 2
    per_owner = (pool + domains - 1) // domains
    vmem, smem = pltpu.VMEM, pltpu.SMEM
    shape = (tiles, comps, half, 2 * width)
    out = jax.ShapeDtypeStruct(shape, jnp.bfloat16)
    block = (comps, half, cells)
    dma = pltpu.SemaphoreType.DMA
    in_vmem = pl.BlockSpec(memory_space=vmem)

    def wide(n):
        return vmem((link_count, -(-n // 128) * 128), jnp.int32)

    both = pl.pallas_call(
        functools.partial(kernel, domains, per_owner),
        out_shape=jax.ShapeDtypeStruct((2,) + shape, jnp.bfloat16),
        in_specs=[pl.BlockSpec(memory_space=pl.ANY)] * 5,
        out_specs=in_vmem,
        scratch_shapes=[
            vmem((1, slot_tile.shape[0]), jnp.int32),
            vmem((1, block_row.shape[0]), jnp.int32),
            vmem((link_count, intersect.shape[0]), jnp.int32),
            vmem(sources.shape, jnp.bfloat16),
            wide(slot_tile.shape[0]),
            wide(block_row.shape[0]),
            wide(intersect.shape[0]),
            smem((domains * per_owner,), jnp.int32),
            smem((domains * per_owner,), jnp.int32),
            smem((domains * per_owner,), jnp.int32),
            vmem((2, links, cells, width), jnp.bfloat16),
            vmem((domains, per_owner) + block, jnp.bfloat16),
            vmem((domains * per_owner,) + block, jnp.bfloat16),
            vmem((tiles, comps * half, 2 * width), jnp.float32),
            vmem((tiles, comps, 2 * width), jnp.float32),
            vmem((tiles, comps, 2 * width), jnp.float32),
            dma((4,)),
            dma((tiles,)),
            dma((domains,)),
            dma((domains,)),
            dma((tiles,)),
            dma((tiles,)),
            dma((2,)),
        ],
        compiler_params=pltpu.CompilerParams(collective_id=0, has_side_effects=True),
        cost_estimate=pl.CostEstimate(
            flops=4 * comps * half * weights.size,
            bytes_accessed=2 * weights.size,
            transcendentals=0,
        ),
    )(
        slot_tile.reshape(1, -1),
        block_row.reshape(1, -1),
        intersect.T,
        sources,
        weights.reshape(links, cells, width),
    )
    return pl.pallas_call(
        deliver,
        out_shape=(out, out),
        in_specs=[in_vmem],
        out_specs=(in_vmem, in_vmem),
    )(both)


def solution(mesh):
    return jax.shard_map(
        shards,
        mesh=mesh,
        in_specs=(P("dom", None, "tm", None), P("dom", None, None, "tm"), P(), P(), P()),
        out_specs=(P("dom", None, "tm", None), P("dom", None, "tm", None)),
        check_vma=False,
    )
```

```python
import functools

import jax
import jax.numpy as jnp
from jax import lax
from jax.experimental import pallas as pl
from jax.experimental.pallas import tpu as pltpu
from jax.sharding import PartitionSpec as P


BIG = 1 << 30


def lookup(table, index):
    lanes = 128
    within, group = index & (lanes - 1), index >> 7
    outs = []
    for at in range(0, index.shape[1], lanes):
        value = jnp.zeros((index.shape[0], lanes), jnp.int32)
        for g in range(table.shape[1] // lanes):
            got = jnp.take_along_axis(
                table[:, g * lanes : (g + 1) * lanes],
                within[:, at : at + lanes],
                axis=1,
                mode="promise_in_bounds",
            )
            value = jnp.where(group[:, at : at + lanes] == g, got, value)
        outs.append(value)
    return outs[0] if len(outs) == 1 else jnp.concatenate(outs, axis=1)


def steps(count, body):
    if count <= 16:
        for i in range(count):
            body(i)
    else:
        def step(i, carry):
            body(i)
            return carry
        lax.fori_loop(0, count, step, 0)


def kernel(
    domains, per_owner,
    tile_hbm, row_hbm, cross_hbm, src_hbm, w_hbm, out_ref,
    tile_ref, row_ref, cross_ref, src_ref,
    wide_tile, wide_row, wide_cross, send_to, link_one, link_two,
    w_ref, pack, buf, acc, edge, beyond,
    in_sem, w_sem, send_sem, recv_sem, wsend_sem, wrecv_sem, edge_sem,
):
    me = lax.axis_index("dom")
    core = lax.axis_index("tm")
    other = 1 - core
    links, width = w_ref.shape[1], w_ref.shape[3]
    blocks, comps, half, cells = src_ref.shape
    tiles = acc.shape[0]
    link_count = links // tiles
    count = comps * half
    mesh_type = pl.DeviceIdType.MESH

    def offset(i):
        return i + 1

    barrier = pltpu.get_barrier_semaphore()

    def greet(i):
        to = lax.rem(me + i + 1, domains)
        pl.semaphore_signal(barrier, inc=1, device_id=(to, core), device_id_type=mesh_type)

    steps(domains - 1, greet)
    pl.semaphore_signal(barrier, inc=1, device_id=(me, other), device_id_type=mesh_type)

    inputs = [
        pltpu.make_async_copy(source, target, in_sem.at[i])
        for i, (source, target) in enumerate(
            (
                (cross_hbm, cross_ref),
                (tile_hbm, tile_ref),
                (row_hbm, row_ref),
                (src_hbm, src_ref),
            )
        )
    ]
    for load in inputs:
        load.start()
    parts = [pl.ds(t * link_count, link_count) for t in range(tiles)]
    loads = [
        pltpu.make_async_copy(w_hbm.at[part], w_ref.at[core, part], w_sem.at[t])
        for t, part in enumerate(parts)
    ]
    for load in loads:
        load.start()

    wide_tile[...] = jnp.zeros_like(wide_tile)
    wide_cross[...] = jnp.zeros_like(wide_cross)
    wide_row[...] = jnp.zeros_like(wide_row)
    for load in inputs[:3]:
        load.wait()
    wide_tile[:, : tile_ref.shape[1]] = jnp.broadcast_to(
        tile_ref[...], (link_count, tile_ref.shape[1])
    )
    wide_cross[:, : cross_ref.shape[1]] = cross_ref[...]
    wide_row[:, : row_ref.shape[1]] = jnp.broadcast_to(
        row_ref[...], (link_count, row_ref.shape[1])
    )
    rows = lookup(wide_row[...], lookup(wide_cross[...], wide_tile[...]))

    slots = rows.shape[1]
    lane = lax.broadcasted_iota(jnp.int32, (1, slots), 1)
    place = lax.rem(lane, tiles)
    local = rows - me * blocks
    mine = (local >= 0) & (local < blocks)
    last = jnp.full((1, slots), -1, jnp.int32)
    for j in range(per_owner):
        least = jnp.min(jnp.where(mine & (local > last), local, BIG), axis=0, keepdims=True)
        joint = least
        for t in range(1, tiles):
            joint = jnp.minimum(joint, pltpu.roll(least, slots - t, 1))
        last = joint
        for t in range(1, tiles):
            last = jnp.where(place == t, pltpu.roll(joint, t, 1), last)
        index = jnp.minimum(last, blocks - 1)
        for d in range(domains):
            send_to[d * per_owner + j] = index[0, d * tiles]

    def fill(d):
        for j in range(per_owner):
            pack[d, j] = src_ref[send_to[d * per_owner + j]]

    inputs[3].wait()
    steps(domains, fill)
    for j in range(per_owner):
        buf[me * per_owner + j] = src_ref[send_to[me * per_owner + j]]

    pl.semaphore_wait(barrier, domains)

    def exchange(to, frm):
        return pltpu.make_async_remote_copy(
            src_ref=pack.at[to],
            dst_ref=buf.at[pl.ds(frm * per_owner, per_owner)],
            send_sem=send_sem.at[to],
            recv_sem=recv_sem.at[frm],
            device_id=(to, core),
            device_id_type=mesh_type,
        )

    def send(i):
        exchange(lax.rem(me + offset(i), domains), me).start()

    steps(domains - 1, send)

    swaps = [
        pltpu.make_async_remote_copy(
            src_ref=w_ref.at[core, part],
            dst_ref=w_ref.at[core, part],
            send_sem=wsend_sem.at[t],
            recv_sem=wrecv_sem.at[t],
            device_id=(me, other),
            device_id_type=mesh_type,
        )
        for t, part in enumerate(parts)
    ]
    for load, swap in zip(loads, swaps):
        load.wait()
        swap.start()

    owners = -(-domains // 128) * 128
    around = lax.broadcasted_iota(jnp.int32, (1, owners), 1)
    owner = around + me
    owner = jnp.where(owner >= domains, owner - domains, owner)
    link = lax.broadcasted_iota(jnp.int32, (link_count, owners), 0)
    locals_ = []
    for t in range(tiles):
        column = jnp.sum(jnp.where(lane == me * tiles + t, rows, 0), axis=1, keepdims=True)
        at = column - owner * blocks
        locals_.append(jnp.where((at >= 0) & (at < blocks), at, BIG))
    last = jnp.full((1, owners), -1, jnp.int32)
    for j in range(per_owner):
        least = [jnp.where(at > last, at, BIG) for at in locals_]
        last = jnp.min(functools.reduce(jnp.minimum, least), axis=0, keepdims=True)
        one = jnp.full((link_count, owners), BIG, jnp.int32)
        two = jnp.full((link_count, owners), -1, jnp.int32)
        for t in range(tiles):
            hit = (locals_[t] == last) & (last < BIG)
            one = jnp.minimum(one, jnp.where(hit, link + t * link_count, BIG))
            two = jnp.maximum(two, jnp.where(hit, link + t * link_count, -1))
        one = jnp.min(one, axis=0, keepdims=True)
        two = jnp.max(two, axis=0, keepdims=True)
        for i in range(domains):
            link_one[i * per_owner + j] = one[0, i]
            link_two[i * per_owner + j] = two[0, i]

    acc[...] = jnp.zeros_like(acc)
    def product(i):
        frm = lax.rem(me + i, domains)
        for j in range(per_owner):
            rows_here = buf[frm * per_owner + j].astype(jnp.float32)
            lhs = rows_here.reshape(count, cells).astype(jnp.bfloat16)
            one = link_one[i * per_owner + j]
            two = link_two[i * per_owner + j]
            at_one, at_two = jnp.minimum(one, links - 1), jnp.maximum(two, 0)
            quad = jnp.concatenate(
                [w_ref[0, at_one], w_ref[1, at_one], w_ref[0, at_two], w_ref[1, at_two]], axis=1
            )
            both = jnp.dot(lhs, quad, preferred_element_type=jnp.float32)
            for t in range(tiles):
                first, end = t * link_count, (t + 1) * link_count
                acc[t] += jnp.where(
                    (one >= first) & (one < end), both[:, : 2 * width], 0.0
                ) + jnp.where((two >= first) & (two < end), both[:, 2 * width :], 0.0)

    def arrive(i):
        frm = lax.rem(me - offset(i) + domains, domains)
        incoming = pltpu.make_async_remote_copy(
            src_ref=pack.at[0],
            dst_ref=buf.at[pl.ds(frm * per_owner, per_owner)],
            send_sem=send_sem.at[frm],
            recv_sem=recv_sem.at[frm],
            device_id=(frm, core),
            device_id_type=mesh_type,
        )
        incoming.wait_recv()

    def weights_in():
        for t, part in enumerate(parts):
            pltpu.make_async_remote_copy(
                src_ref=w_hbm.at[part],
                dst_ref=w_ref.at[other, part],
                send_sem=wsend_sem.at[t],
                recv_sem=wrecv_sem.at[t],
                device_id=(me, other),
                device_id_type=mesh_type,
            ).wait_recv()

    weights_in()
    product(0)
    if domains <= 16:
        for i in range(domains - 1):
            arrive(i)
            product(domains - offset(i))
    else:
        steps(domains - 1, arrive)
        steps(domains - 1, lambda i: product(i + 1))

    total = acc[...].reshape(tiles, comps, half, 2 * width)
    edge[...] = jnp.where(core == 0, total[:, :, half - 1], total[:, :, 0])
    halo = pltpu.make_async_remote_copy(
        src_ref=edge,
        dst_ref=beyond,
        send_sem=edge_sem.at[0],
        recv_sem=edge_sem.at[1],
        device_id=(me, other),
        device_id_type=mesh_type,
    )
    out_ref[0] = total.astype(jnp.bfloat16)

    def drain(i):
        exchange(lax.rem(me + i + 1, domains), me).wait_send()

    steps(domains - 1, drain)
    for swap in swaps:
        swap.wait_send()
    halo.start()
    halo.wait()
    sample = lax.broadcasted_iota(jnp.int32, (half, 2 * width), 0)
    for t in range(tiles):
        for p in range(comps):
            here = total[t, p]
            outer = jnp.broadcast_to(beyond[t, pl.ds(p, 1)], here.shape)
            later = pltpu.roll(here, half - 1, 0)
            prior = pltpu.roll(here, 1, 0)
            later = jnp.where((sample == half - 1) & (core == 0), outer, later)
            prior = jnp.where((sample == 0) & (core == 1), outer, prior)
            rate = jnp.where(
                (sample == 0) & (core == 0),
                later - here,
                jnp.where(
                    (sample == half - 1) & (core == 1), here - prior, (later - prior) * 0.5
                ),
            )
            out_ref[1, t, p] = rate.astype(jnp.bfloat16)


def deliver(both_ref, source_ref, rate_ref):
    source_ref[...] = both_ref[0]
    rate_ref[...] = both_ref[1]


def shards(sources, weights, intersect, block_row, slot_tile):
    domains = lax.axis_size("dom")
    tiles, link_count, cells, width = weights.shape
    blocks, comps, half, _ = sources.shape
    links = tiles * link_count
    pool = links // 2
    per_owner = (pool + domains - 1) // domains
    vmem, smem = pltpu.VMEM, pltpu.SMEM
    shape = (tiles, comps, half, 2 * width)
    out = jax.ShapeDtypeStruct(shape, jnp.bfloat16)
    block = (comps, half, cells)
    dma = pltpu.SemaphoreType.DMA
    in_vmem = pl.BlockSpec(memory_space=vmem)

    def wide(n):
        return vmem((link_count, -(-n // 128) * 128), jnp.int32)

    both = pl.pallas_call(
        functools.partial(kernel, domains, per_owner),
        out_shape=jax.ShapeDtypeStruct((2,) + shape, jnp.bfloat16),
        in_specs=[pl.BlockSpec(memory_space=pl.ANY)] * 5,
        out_specs=in_vmem,
        scratch_shapes=[
            vmem((1, slot_tile.shape[0]), jnp.int32),
            vmem((1, block_row.shape[0]), jnp.int32),
            vmem((link_count, intersect.shape[0]), jnp.int32),
            vmem(sources.shape, jnp.bfloat16),
            wide(slot_tile.shape[0]),
            wide(block_row.shape[0]),
            wide(intersect.shape[0]),
            smem((domains * per_owner,), jnp.int32),
            smem((domains * per_owner,), jnp.int32),
            smem((domains * per_owner,), jnp.int32),
            vmem((2, links, cells, width), jnp.bfloat16),
            vmem((domains, per_owner) + block, jnp.bfloat16),
            vmem((domains * per_owner,) + block, jnp.bfloat16),
            vmem((tiles, comps * half, 2 * width), jnp.float32),
            vmem((tiles, comps, 2 * width), jnp.float32),
            vmem((tiles, comps, 2 * width), jnp.float32),
            dma((4,)),
            dma((tiles,)),
            dma((domains,)),
            dma((domains,)),
            dma((tiles,)),
            dma((tiles,)),
            dma((2,)),
        ],
        compiler_params=pltpu.CompilerParams(collective_id=0, has_side_effects=True),
        cost_estimate=pl.CostEstimate(
            flops=4 * comps * half * weights.size,
            bytes_accessed=2 * weights.size,
            transcendentals=0,
        ),
    )(
        slot_tile.reshape(1, -1),
        block_row.reshape(1, -1),
        intersect.T,
        sources,
        weights.reshape(links, cells, width),
    )
    return pl.pallas_call(
        deliver,
        out_shape=(out, out),
        in_specs=[in_vmem],
        out_specs=(in_vmem, in_vmem),
    )(both)


def solution(mesh):
    return jax.shard_map(
        shards,
        mesh=mesh,
        in_specs=(P("dom", None, "tm", None), P("dom", None, None, "tm"), P(), P(), P()),
        out_specs=(P("dom", None, "tm", None), P("dom", None, "tm", None)),
        check_vma=False,
    )
```
